32 devices in a mesh: cons: 4 (over y, x), blk: 8 (over z, core).
Axes of the slice: x: 2, y: 2, z: 4, core: 2. Of those that a mesh axis runs over, the one named last changes fastest.
Arguments:
- elevation: bfloat16 [16, 320, 6144], P('cons', 'blk'), may hold values from -6 to 6
- legendre: bfloat16 [320, 768, 768], P('blk', 'cons'), may hold values from -5 to 5, as said below
- cycle_weight: float32 [320], P('blk'), may hold values from 0.0003565902 to 0.0028527216
- love_factor: float32 [768], replicated, may hold values from 0.000390625 to 0.0052083335
- assignment: int32 [16], replicated, may hold values from 0 to 15, each once
Outputs:
- loading: float32 [16, 320, 6144], P('cons', 'blk')
The draws below stay inside these ranges and needn't reach their ends.
Inputs may be any that keep to these rules, and one draw needn't show every extreme that they name: `legendre`: fully normalized associated Legendre functions (the square integrates to 1 over [-1, 1]) of each cycle's latitude, every cycle within 26 degrees of the equator; zero where the degree is below the order.
All inputs are finite; a program needn't handle non-finite values.
Results may differ from the reference program's by a relative error of at most 0.02.
Values may be sent and summed in bfloat16 or wider, within the bound.
A program may use at most 128 MiB of HBM per device.

```python
import math
import jax
import jax.numpy as jnp
from jax import lax

FIELDS = 16
DEGREES = 768
ORDERS = 768
LONS = 6144
CYCLE_DEV = 40
CYCLES = 320
N_BLK = 8


def draw_legendre(key, part):
    cosine_vals = jax.random.uniform(jax.random.fold_in(key, 11), (CYCLES,), jnp.float32, -0.43, 0.43)
    sine_vals = jnp.sqrt(1.0 - cosine_vals * cosine_vals)
    order_vals = jnp.arange(ORDERS).astype(jnp.float32)
    growth = 0.5 * jnp.log((2.0 * order_vals + 1.0) / jnp.maximum(2.0 * order_vals, 1.0))
    log_steps = jnp.where(order_vals[None, :] > 0.0, growth[None, :] + jnp.log(sine_vals)[:, None], 0.0)
    diagonal = jnp.exp(0.5 * jnp.log(0.5) + jnp.cumsum(log_steps, axis=1))
    order_sq = order_vals[None, :] * order_vals[None, :]

    def advance(state, degree):
        previous, earlier = state
        level = degree.astype(jnp.float32)
        coef_now = jnp.sqrt((4.0 * level * level - 1.0) / jnp.maximum(level * level - order_sq, 1.0))
        lower = level - 1.0
        coef_before = jnp.sqrt(jnp.maximum(4.0 * lower * lower - 1.0, 1.0) / jnp.maximum(lower * lower - order_sq, 1.0))
        generic = coef_now * (cosine_vals[:, None] * previous - earlier / coef_before)
        first_up = jnp.sqrt(2.0 * order_vals[None, :] + 3.0) * cosine_vals[:, None] * previous
        values = jnp.where(level == order_vals[None, :], diagonal, jnp.where(level == order_vals[None, :] + 1.0, first_up, jnp.where(level > order_vals[None, :] + 1.0, generic, 0.0)))
        return ((values, previous), values)
    zeros = jnp.zeros((CYCLES, ORDERS), jnp.float32)
    _, table = lax.scan(advance, (zeros, zeros), jnp.arange(DEGREES, dtype=jnp.int32))
    return jnp.transpose(table, (1, 2, 0)).astype(jnp.bfloat16)


def level_of(own_key, dims, shards, smallest, high):
    def one(dim, shards_of):
        steps = jax.random.uniform(jax.random.fold_in(jax.random.fold_in(own_key, 6), dim), (shards_of,), jnp.float32, smallest / len(shards), high / len(shards))
        return jnp.repeat(jnp.exp(steps), dims[dim] // shards_of).reshape((-1,) + (1,) * (len(dims) - dim - 1))

    level = one(*shards[0])
    for cut in shards[1:]:
        level = level * one(*cut)
    return level


def normal_values(own_key, dims, deviation, bound, split=(), kind=jnp.bfloat16):
    entries = jax.random.normal(own_key, dims, jnp.float32) * deviation
    if len(split) > 0:
        entries = level_of(own_key, dims, split, -0.22, 0.18) * entries
    return jnp.clip(entries, min=-bound, max=bound).astype(kind)


def setup_inputs(seed: int = 0) -> dict:
    keys = jax.random.split(jax.random.key(seed), 6)
    return {
        "elevation": normal_values(keys[0], (FIELDS, CYCLES, LONS), 1.0, 6.0, ((0, 4), (1, 8))),
        "legendre": draw_legendre(jax.random.fold_in(keys[5], 71), 0),
        "cycle_weight": jnp.clip(jnp.exp(math.log(0.0028527216) - 2.0794415 * jax.random.uniform(keys[2], (CYCLES,), jnp.float32) ** level_of(keys[2], (CYCLES,), ((0, 8),), -0.2, 0.2)), 0.0003565902, 0.0028527216),
        "love_factor": jnp.clip(jnp.exp(jax.random.uniform(keys[3], (DEGREES,), jnp.float32, math.log(0.000390625), math.log(0.0052083335))), 0.000390625, 0.0052083335),
        "assignment": jax.random.permutation(keys[4], FIELDS).astype(jnp.int32),
    }


def fourier_block(offset, length, period, orders):
    lon_index = offset + jnp.arange(length, dtype=jnp.int32)
    order_index = jnp.arange(orders, dtype=jnp.int32)
    phases = (lon_index[:, None] * order_index[None, :]) % period
    angles = phases.astype(jnp.float32) * jnp.float32(2.0 * 3.141592653589793 / period)
    stacked = jnp.stack([jnp.cos(angles), -jnp.sin(angles)], axis=2)
    return stacked.reshape(length, 2 * orders).astype(jnp.bfloat16)


def reference(elevation, legendre, cycle_weight, love_factor, assignment):
    table = fourier_block(0, LONS, LONS, ORDERS)

    def forward(field):
        summed = jnp.dot(field, table, preferred_element_type=jnp.float32)
        return (summed * cycle_weight[:, None]).astype(jnp.bfloat16)

    spectra = lax.map(forward, elevation)
    ordered = spectra[assignment].reshape(FIELDS, CYCLES, ORDERS, 2)

    def add_block(running, block_index):
        start = (block_index * CYCLE_DEV).astype(jnp.int32)
        values = lax.dynamic_slice_in_dim(legendre, start, CYCLE_DEV, 0).astype(jnp.float32)
        spec_block = lax.dynamic_slice_in_dim(ordered, start, CYCLE_DEV, 1).astype(jnp.float32)
        partial_value = jnp.einsum('jml,gjmp->lpgm', values, spec_block)
        rounded = lax.optimization_barrier(partial_value.astype(jnp.bfloat16))
        return running + rounded.astype(jnp.float32), None

    zeros = jnp.zeros((DEGREES, 2, FIELDS, ORDERS), jnp.float32)
    analysis, _ = lax.scan(add_block, zeros, jnp.arange(N_BLK, dtype=jnp.int32))
    coefficients = (analysis * love_factor[:, None, None, None]).astype(jnp.bfloat16)
    order_factor = jnp.where(jnp.arange(ORDERS) == 0, 1.0, 2.0).astype(jnp.float32)

    def synth_block(block_index):
        start = (block_index * CYCLE_DEV).astype(jnp.int32)
        values = lax.dynamic_slice_in_dim(legendre, start, CYCLE_DEV, 0).astype(jnp.float32)
        summed = jnp.einsum('jml,lpgm->gjmp', values, coefficients.astype(jnp.float32))
        return (summed * order_factor[None, None, :, None]).astype(jnp.bfloat16)

    blocks = lax.map(synth_block, jnp.arange(N_BLK, dtype=jnp.int32))
    synthesis = jnp.moveaxis(blocks, 0, 1).reshape(FIELDS, CYCLES, 2 * ORDERS)

    def inverse(field):
        return jnp.dot(field, table.T, preferred_element_type=jnp.float32)

    return lax.map(inverse, synthesis)
```

```python
import functools

import jax
import jax.numpy as jnp
from jax import lax
from jax.experimental import pallas as pl
from jax.experimental.pallas import tpu as pltpu
from jax.sharding import PartitionSpec as P

PIECE_ROWS = 128


def chain_kernel(n, x_ref, out_ref, held, sum_send, sum_recv, back_send, back_recv):
    me = lax.axis_index("blk")
    pieces = x_ref.shape[1]
    up, down = lax.rem(me + 1, n), lax.rem(me + n - 1, n)
    barrier = pltpu.get_barrier_semaphore()
    for neighbour in (up, down):
        pl.semaphore_signal(
            barrier, inc=1, device_id={"blk": neighbour}, device_id_type=pl.DeviceIdType.MESH
        )
    pl.semaphore_wait(barrier, 2)
    places = (me, n - 1 - me)
    nexts, befores = (up, down), (down, up)

    def forward(h, src, c):
        return pltpu.make_async_remote_copy(
            src_ref=src,
            dst_ref=held.at[h, c],
            send_sem=sum_send.at[h, c],
            recv_sem=sum_recv.at[h, c],
            device_id={"blk": nexts[h]},
            device_id_type=pl.DeviceIdType.MESH,
        )

    def backward(h, c):
        return pltpu.make_async_remote_copy(
            src_ref=out_ref.at[h, c],
            dst_ref=out_ref.at[h, c],
            send_sem=back_send.at[h, c],
            recv_sem=back_recv.at[h, c],
            device_id={"blk": befores[h]},
            device_id_type=pl.DeviceIdType.MESH,
        )

    def total(h, c):
        both = held[h, c].astype(jnp.float32) + x_ref[h, c].astype(jnp.float32)
        return both.astype(out_ref.dtype)

    for h in range(2):

        @pl.when(places[h] == 0)
        def _():
            def begin(c, carry):
                forward(h, x_ref.at[h, c], c).start()
                return carry

            lax.fori_loop(0, pieces, begin, 0)

    def sum_step(i, carry):
        for h in range(2):
            c = i - places[h]

            @pl.when((places[h] > 0) & (c >= 0) & (c < pieces))
            def _():
                forward(h, held.at[h, c], c).wait_recv()

                @pl.when(places[h] < n - 1)
                def _():
                    held[h, c] = total(h, c)
                    forward(h, held.at[h, c], c).start()

                @pl.when(places[h] == n - 1)
                def _():
                    out_ref[h, c] = total(h, c)
                    backward(h, c).start()

        return carry

    lax.fori_loop(0, pieces + n - 1, sum_step, 0)

    def back_step(i, carry):
        for h in range(2):
            c = i - (n - 1 - places[h])

            @pl.when((places[h] < n - 1) & (c >= 0) & (c < pieces))
            def _():
                backward(h, c).wait_recv()

                @pl.when(places[h] > 0)
                def _():
                    backward(h, c).start()

        return carry

    lax.fori_loop(0, pieces + n - 1, back_step, 0)

    def drain(c, carry):
        for h in range(2):

            @pl.when(places[h] < n - 1)
            def _():
                forward(h, held.at[h, c], c).wait_send()

            @pl.when(places[h] > 0)
            def _():
                backward(h, c).wait_send()

        return carry

    lax.fori_loop(0, pieces, drain, 0)


def chain_sum(rows, n):
    count, lanes = rows.shape
    shape = (2, count // (2 * PIECE_ROWS), PIECE_ROWS, lanes)
    out = pl.pallas_call(
        functools.partial(chain_kernel, n),
        out_shape=jax.ShapeDtypeStruct(shape, rows.dtype),
        in_specs=[pl.BlockSpec(memory_space=pltpu.VMEM)],
        out_specs=pl.BlockSpec(memory_space=pltpu.VMEM),
        scratch_shapes=[pltpu.VMEM(shape, rows.dtype)]
        + [pltpu.SemaphoreType.DMA(shape[:2])] * 4,
        compiler_params=pltpu.CompilerParams(collective_id=0, has_side_effects=True),
    )(rows.reshape(shape))
    return out.reshape(count, lanes)


def angles_of(lon_index, period, orders):
    order_index = jnp.arange(orders, dtype=jnp.int32)
    phases = lon_index[:, None] * order_index[None, :] % period
    angles = phases.astype(jnp.float32) * jnp.float32(2.0 * 3.141592653589793 / period)
    return jnp.cos(angles), jnp.sin(angles)


def quarter_table(length, period, orders):
    fine = 32
    coarse = length // fine
    parts = angles_of(jnp.arange(coarse, dtype=jnp.int32) * fine, period, orders)
    parts += angles_of(jnp.arange(fine, dtype=jnp.int32), period, orders)
    cos_a, sin_a, cos_b, sin_b = lax.optimization_barrier(parts)
    cos_a, sin_a = cos_a[:, None, :], sin_a[:, None, :]
    cosine = cos_a * cos_b[None] - sin_a * sin_b[None]
    minus_sine = -(sin_a * cos_b[None] + cos_a * sin_b[None])
    both = jnp.concatenate([cosine.astype(jnp.bfloat16), minus_sine.astype(jnp.bfloat16)], axis=2)
    return both.reshape(length, 2 * orders)


def local(elevation, legendre, cycle_weight, love_factor, assignment):
    fld_dev, cycle_dev, longitudes = elevation.shape
    orders_dev, degrees = legendre.shape[1:]
    orders = orders_dev * lax.axis_size("cons")
    quarter = longitudes // 4
    table = lax.optimization_barrier(quarter_table(quarter, longitudes, orders))
    residue = jnp.arange(orders, dtype=jnp.int32) % 4
    turn_re = (residue == 0).astype(jnp.float32) - (residue == 2).astype(jnp.float32)
    turn_im = (residue == 1).astype(jnp.float32) - (residue == 3).astype(jnp.float32)
    sign = turn_re * turn_re - turn_im * turn_im

    def halves(q):
        part = lax.slice_in_dim(elevation, q * quarter, (q + 1) * quarter, axis=2)
        both = jnp.einsum("fjk,kn->fjn", part, table, preferred_element_type=jnp.float32)
        return both[..., :orders], both[..., orders:]

    (re0, im0), (re1, im1), (re2, im2), (re3, im3) = (halves(q) for q in range(4))
    even_re, even_im = re0 + sign * re2, im0 + sign * im2
    odd_re, odd_im = re1 + sign * re3, im1 + sign * im3
    running = jnp.stack(
        [
            even_re + turn_re * odd_re + turn_im * odd_im,
            even_im + turn_re * odd_im - turn_im * odd_re,
        ],
        axis=1,
    )
    spectra = (running * cycle_weight[None, None, :, None]).astype(jnp.bfloat16)
    moved = lax.all_to_all(spectra, "cons", split_axis=3, concat_axis=0, tiled=True)
    fields = moved.shape[0]
    one_hot = (assignment[:, None] == jnp.arange(fields, dtype=jnp.int32)[None, :]).astype(
        jnp.bfloat16
    )
    ordered = jnp.einsum(
        "gf,fpjm->gpjm", one_hot, moved, preferred_element_type=jnp.float32
    ).astype(jnp.bfloat16)
    slots = ordered.reshape(2 * fields, cycle_dev, orders_dev)
    partial = jnp.einsum(
        "jml,rjm->mrl", legendre, slots, preferred_element_type=jnp.float32
    ).astype(jnp.bfloat16)
    whole = chain_sum(
        partial.reshape(orders_dev * fields * 2, degrees), lax.axis_size("blk")
    ).reshape(orders_dev, fields * 2, degrees)
    coefficients = (whole.astype(jnp.float32) * love_factor).astype(jnp.bfloat16)
    order_index = lax.axis_index("cons") * orders_dev + jnp.arange(orders_dev, dtype=jnp.int32)
    order_factor = jnp.where(order_index == 0, 1.0, 2.0).astype(jnp.float32)
    summed = jnp.einsum(
        "jml,mrl->rjm", legendre, coefficients, preferred_element_type=jnp.float32
    )
    synthesis = (summed * order_factor).astype(jnp.bfloat16)
    synthesis = synthesis.reshape(fields, 2, cycle_dev, orders_dev)
    returned = lax.all_to_all(synthesis, "cons", split_axis=0, concat_axis=3, tiled=True)
    re, im = returned[:, 0].astype(jnp.float32), returned[:, 1].astype(jnp.float32)
    turned = [
        (re, im),
        (turn_re * re - turn_im * im, turn_re * im + turn_im * re),
        (sign * re, sign * im),
        (turn_re * re + turn_im * im, turn_re * im - turn_im * re),
    ]
    return jnp.concatenate(
        [
            jnp.einsum(
                "fjn,kn->fjk",
                jnp.concatenate(pair, axis=2).astype(jnp.bfloat16),
                table,
                preferred_element_type=jnp.float32,
            )
            for pair in turned
        ],
        axis=2,
    )


def solution(mesh):
    placed = (P("cons", "blk", None), P("blk", "cons", None), P("blk"), P(), P())
    return jax.shard_map(
        local, mesh=mesh, in_specs=placed, out_specs=P("cons", "blk", None), check_vma=False
    )
```
